32 devices in a mesh: grp: 16 (over z, y, core), row: 2 (over x).
Axes of the slice: x: 2, y: 2, z: 4, core: 2. Of those that a mesh axis runs over, the one named last changes fastest.
Arguments:
- vectors: float32 [1536, 16384], P('grp', 'row'), may hold values from -1.002 to 1.002, as said below
- diagonal: float32 [16384], replicated, may hold values from -2 to 2
- off_diag: float32 [16384], replicated, may hold values from -1 to 1
- eigen: float32 [1536], P('grp'), may hold values from -3 to 3
Outputs:
- orth_ratio: float32 [1536], P('grp')
- resid_norm: float32 [1536], P('grp')
- scaled_resid: float32 [1536, 16384], P('grp', 'row')
- worst: float32 [2], replicated
The draws below stay inside these ranges and needn't reach their ends.
Inputs may be any that keep to these rules, and one draw needn't show every extreme that they name: Each row of vectors has Euclidean norm between 0.998 and 1.002.
All inputs are finite; a program needn't handle non-finite values.
Results may differ from the reference program's by a relative error of at most 0.00011.
Values sent between devices are 32-bit elements; how exact they have to be, the bound alone decides.
No kernel may reach another device: no remote copies, remote signals or barrier semaphores. Data moves between devices by JAX's collectives and lax.ppermute only.
A program may use at most 64 MiB of HBM per device.

```python
import jax
import jax.numpy as jnp
from jax import lax

N = 16384
K = 1536


def draw_vectors(key, part):
    first = jax.random.fold_in(key, 11)
    third = jax.random.fold_in(key, 37)
    raw = jax.random.normal(first, (K, N), jnp.float32)
    lengths = jnp.sqrt(jnp.sum(raw * raw, axis=1, keepdims=True))
    stretch = 1.0 + jax.random.uniform(third, (K, 1), jnp.float32, -0.002, 0.002)
    return (raw / lengths * stretch).astype(jnp.float32)


def steps_of(own_key, shape, shards, least, largest):
    def one(dim, shards_of):
        heights = jax.random.uniform(jax.random.fold_in(jax.random.fold_in(own_key, 6), dim), (shards_of,), jnp.float32, least / len(shards), largest / len(shards))
        return jnp.repeat(jnp.exp(heights), shape[dim] // shards_of).reshape((-1,) + (1,) * (len(shape) - dim - 1))

    gain = one(*shards[0])
    for cut in shards[1:]:
        gain = gain * one(*cut)
    return gain


def setup_inputs(seed: int = 0) -> dict:
    key_list = jax.random.split(jax.random.key(seed), 5)
    vectors = draw_vectors(jax.random.fold_in(key_list[4], 71), 0)
    diagonal = jnp.clip(jax.random.uniform(key_list[1], (N,), jnp.float32, -2.0, 2.0), -2.0, 2.0)
    off_diag = jnp.clip(jax.random.uniform(key_list[2], (N,), jnp.float32, -1.0, 1.0), -1.0, 1.0)
    eigen = jnp.clip(jax.random.uniform(key_list[3], (K,), jnp.float32, -3.0, 3.0) * steps_of(key_list[3], (K,), ((0, 16),), -0.4, 0.0), -3.0, 3.0)
    return {"vectors": vectors, "diagonal": diagonal, "off_diag": off_diag, "eigen": eigen}


def reference(vectors, diagonal, off_diag, eigen):
    gram = jnp.dot(vectors, vectors.T, precision=lax.Precision.HIGHEST, preferred_element_type=jnp.float32)
    count = gram.shape[0]
    deviation = jnp.abs(gram - jnp.eye(count, dtype=jnp.float32))
    scale = jnp.sqrt(jnp.float32(N))
    orth_ratio = scale * lax.optimization_barrier(jnp.max(deviation, axis=1))
    padded = jnp.pad(vectors, ((0, 0), (1, 1)))
    before = jnp.concatenate([jnp.zeros((1,), jnp.float32), off_diag[:-1]])
    resid = diagonal * vectors + before * padded[:, :-2] + off_diag * padded[:, 2:] - eigen[:, None] * vectors
    scaled_resid = scale * resid
    resid_norm = jnp.sqrt(lax.optimization_barrier(jnp.sum(resid * resid, axis=1)))
    worst = jnp.stack([jnp.max(orth_ratio), jnp.max(resid_norm)])
    return (orth_ratio, resid_norm, scaled_resid, worst)
```

```python
import math

import jax
import jax.numpy as jnp
from jax import lax
from jax.sharding import PartitionSpec as P

N = 16384
SHARES = (3, 2, 1)


def cuts_of(width):
    unit = width // sum(SHARES)
    sizes = [unit * share for share in SHARES[:-1]]
    sizes.append(width - sum(sizes))
    starts = [sum(sizes[:i]) for i in range(len(sizes))]
    return list(zip(starts, sizes))


def swapped(array, axis, distance):
    size = lax.axis_size(axis)
    return lax.ppermute(array, axis, [(i, i ^ distance) for i in range(size)])


def largest_over(array, axis, distances):
    return [swapped(array, axis, distance) for distance in distances]


def total_over(array, axis):
    distance = 1
    while distance < lax.axis_size(axis):
        array = array + swapped(array, axis, distance)
        distance *= 2
    return array


def block_gram(left, right):
    return lax.dot_general(
        left,
        right,
        (((1,), (1,)), ((), ())),
        precision=lax.Precision.HIGH,
        preferred_element_type=jnp.float32,
    )


def residual(vectors, diagonal, off_diag, eigen):
    size = lax.axis_size("row")
    seg_rows = vectors.shape[1]
    start = lax.axis_index("row") * seg_rows
    up = [(i, i + 1) for i in range(size - 1)]
    down = [(j, i) for i, j in up]
    before = lax.ppermute(vectors[:, -1:], "row", up)
    after = lax.ppermute(vectors[:, :1], "row", down)
    padded = jnp.concatenate([before, vectors, after], axis=1)
    local_diag = lax.dynamic_slice_in_dim(diagonal, start, seg_rows)
    local_off = lax.dynamic_slice_in_dim(off_diag, start, seg_rows)
    shifted_off = jnp.concatenate([jnp.zeros((1,), jnp.float32), off_diag])
    local_before = lax.dynamic_slice_in_dim(shifted_off, start, seg_rows)
    resid = (
        local_diag * vectors
        + local_before * padded[:, :-2]
        + local_off * padded[:, 2:]
        - eigen[:, None] * vectors
    )
    squares = total_over(jnp.sum(resid * resid, axis=1), "row")
    return resid, jnp.sqrt(squares)


def shards(vectors, diagonal, off_diag, eigen):
    scale = jnp.float32(math.sqrt(N))
    width, seg_rows = vectors.shape
    groups, members = lax.axis_size("grp"), lax.axis_size("row")
    near = 4
    far = groups // near
    plane = lax.axis_index("grp") // near
    here = lax.axis_index("row")
    cols = seg_rows // far
    cuts = cuts_of(width)

    arrived = []
    for start, size in cuts:
        pieces = []
        for k in range(far):
            piece = lax.dynamic_slice(vectors, (start, (plane ^ k) * cols), (size, cols))
            pieces.append(swapped(piece, "grp", k * near) if k else piece)
        arrived.append(pieces)

    resid, resid_norm = residual(vectors, diagonal, off_diag, eigen)
    scaled_resid = scale * resid

    blocks = []
    tops = [None] * len(cuts)
    own_tops = []
    for i, (start, size) in enumerate(cuts):
        own = jnp.zeros((far * size, cols), jnp.float32)
        for k in range(far):
            own = lax.dynamic_update_slice(own, arrived[i][k], ((plane ^ k) * size, 0))
        held = {0: own}
        distance = near // 2
        while distance:
            for d in list(held):
                held[d ^ distance] = swapped(held[d], "grp", distance)
            distance //= 2
        blocks.append(jnp.concatenate([held[d] for d in range(near)], axis=0))
        own_top = None
        for j in range(i + 1):
            part = block_gram(own, blocks[j])
            share = part.shape[1] // members

            def columns_of(r):
                return lax.dynamic_slice_in_dim(part, r * share, share, axis=1)

            mine = columns_of(here)
            for r in range(1, members):
                mine = mine + swapped(columns_of(here ^ r), "row", r)

            def rows_of(p):
                return lax.dynamic_slice_in_dim(mine, p * size, size, axis=0)

            final = rows_of(plane)
            for k in range(1, far):
                final = final + swapped(rows_of(plane ^ k), "grp", k * near)
            if j == i:
                row_ids = plane * size + lax.broadcasted_iota(jnp.int32, final.shape, 0)
                col_ids = here * share + lax.broadcasted_iota(jnp.int32, final.shape, 1)
                final = final - (row_ids == col_ids).astype(jnp.float32)
            final = jnp.abs(final)
            row_top = jnp.max(final, axis=1)
            col_top = jnp.max(final, axis=0)
            own_top = row_top if own_top is None else jnp.maximum(own_top, row_top)
            tops[j] = col_top if tops[j] is None else jnp.maximum(tops[j], col_top)
        own_tops.append(own_top)

    table = []
    for (start, size), col_top, own_top in zip(cuts, tops, own_tops):
        whole = jnp.zeros((near * far * size,), jnp.float32)
        whole = lax.dynamic_update_slice(whole, col_top, (here * col_top.shape[0],))
        whole = whole.reshape(near, far, size)
        first = lax.dynamic_update_slice(
            jnp.zeros((far, size), jnp.float32), own_top[None], (plane, 0)
        )
        table.append(whole.at[0].max(first))
    table = jnp.concatenate(table, axis=2).reshape(near * far, width)
    resid_top = jnp.max(resid_norm)
    packed = jnp.concatenate([table.reshape(-1), resid_top[None]])
    distance = 1
    while distance < members:
        packed = jnp.maximum(packed, swapped(packed, "row", distance))
        distance *= 2
    for other in largest_over(packed, "grp", [k * near for k in range(1, far)]):
        packed = jnp.maximum(packed, other)
    resid_top = packed[-1]
    table = packed[:-1].reshape(near, far, width)
    orth_top = jnp.max(table)
    kept = lax.dynamic_slice_in_dim(table, plane, 1, axis=1)[:, 0]
    extra = jnp.stack([orth_top, resid_top])
    result = jnp.concatenate([kept[0], extra])
    for d in range(1, near):
        other = swapped(jnp.concatenate([kept[d], extra]), "grp", d)
        result = jnp.maximum(result, other)
    orth_ratio = scale * result[:width]
    worst = jnp.stack([scale * result[width], result[width + 1]])
    return (orth_ratio, resid_norm, scaled_resid, worst)


def solution(mesh):
    placed = (P("grp", "row"), P(), P(), P("grp"))
    return jax.shard_map(
        shards,
        mesh=mesh,
        in_specs=placed,
        out_specs=(P("grp"), P("grp"), P("grp", "row"), P()),
        check_vma=False,
    )
```
